32 devices in a mesh: group: 4 (over y, core), local: 8 (over z, x).
Axes of the slice: x: 2, y: 2, z: 4, core: 2. Of those that a mesh axis runs over, the one named last changes fastest.
Arguments:
- lookup_grads: bfloat16 [262144, 256], P(('group', 'local')), may hold values from -0.29882812 to 0.29882812
- slot_index: int32 [2, 262144], P(None, ('group', 'local')), may hold values from 0 to 511, as said below
- unique_rows: int32 [2, 2048], P(None, ('group', 'local')), may hold values from -1 to 32767, as said below
- tables: float32 [2, 32768, 256], P(None, ('group', 'local')), may hold values from -6 to 6
- accums: float32 [2, 32768], P(None, ('group', 'local')), may hold values from 0.01 to 1
Outputs:
- new_tables: float32 [2, 32768, 256], P(None, ('group', 'local'))
- new_accums: float32 [2, 32768], P(None, ('group', 'local'))
The draws below stay inside these ranges and needn't reach their ends.
Inputs may be any that keep to these rules, and one draw needn't show every extreme that they name: slot_index[t, i] names a slot of lookup i's group list whose entry in unique_rows[t] is not -1. `unique_rows`: table row p is owned by device p // 1024, which is device (group p // 8192, local p // 1024 % 8). Group g's list is entries g * 512 to (g + 1) * 512 - 1; its block l of 64 entries consists of 4 buckets of 16 entries, bucket h holding only rows owned by device (group h, local l), the used entries first and -1 after them. Rows within a group's list are distinct. In every draw and table some device (group h, local l) gets a full bucket from every group.
All inputs are finite; a program needn't handle non-finite values.
Results may differ from the reference program's by a relative error of at most 0.0003.
Values sent between devices are 32-bit elements; how exact they have to be, the bound alone decides.
A program may use at most 64 MiB of HBM per device.

```python
import math
import jax
import jax.numpy as jnp
from jax import lax

EMB = 256
LOOK_DEV = 8192
CAP = 16
ROWS_DEV = 1024
SLOTS = 64
GROUP_SLOTS = 512
ALL_SLOTS = 2048
LOOKUPS = 262144
ROWS = 32768
N_GROUP = 4
N_LOCAL = 8


def shared_layout(key):
    base_key = jax.random.fold_in(key, 7)
    count_key, pick_key, offset_key, stride_key = jax.random.split(base_key, 4)
    bucket_shape = (2, N_GROUP, N_LOCAL, N_GROUP)
    live_count = jax.random.randint(count_key, bucket_shape, (CAP + 3) // 4, CAP + 1)
    local_pick = jax.random.randint(jax.random.fold_in(pick_key, 1), (2,), 0, N_LOCAL)
    group_pick = jax.random.randint(jax.random.fold_in(pick_key, 2), (2,), 0, N_GROUP)
    local_iota = jnp.arange(N_LOCAL)[None, None, :, None]
    group_iota = jnp.arange(N_GROUP)[None, None, None, :]
    marked = (local_iota == local_pick[:, None, None, None]) & (group_iota == group_pick[:, None, None, None])
    live_count = jnp.where(marked, CAP, live_count)
    return (live_count, offset_key, stride_key)


def draw_unique_rows(key, part):
    live_count, offset_key, stride_key = shared_layout(key)
    bucket_shape = (2, N_GROUP, N_LOCAL, N_GROUP)
    offset = jax.random.randint(offset_key, bucket_shape, 0, ROWS_DEV)
    stride = 2 * jax.random.randint(stride_key, bucket_shape, 0, max(ROWS_DEV // 2, 1)) + 1
    position = jnp.arange(CAP)
    local_rows = (offset[..., None] + stride[..., None] * position) % ROWS_DEV
    owners = jnp.arange(N_GROUP)[None, None, None, :] * N_LOCAL + jnp.arange(N_LOCAL)[None, None, :, None]
    row_ids = owners[..., None] * ROWS_DEV + local_rows
    row_ids = jnp.where(position < live_count[..., None], row_ids, -1)
    return row_ids.reshape(2, ALL_SLOTS).astype(jnp.int32)


def draw_slot_index(key, part):
    live_count, offset_key, stride_key = shared_layout(key)
    slot_key = jax.random.fold_in(key, 19)
    first_key, second_key, third_key = jax.random.split(slot_key, 3)
    local_choice = jax.random.randint(first_key, (2, LOOKUPS), 0, N_LOCAL)
    group_choice = jax.random.randint(second_key, (2, LOOKUPS), 0, N_GROUP)
    random_bits = jax.random.randint(third_key, (2, LOOKUPS), 0, 2 ** 20)
    group_of = jnp.arange(LOOKUPS) // (LOOK_DEV * N_LOCAL)
    table_of = jnp.arange(2)[:, None]
    available = live_count[table_of, group_of[None, :], local_choice, group_choice]
    slots = local_choice * SLOTS + group_choice * CAP + random_bits % available
    return slots.astype(jnp.int32)


def block_scale(key, shape, pieces, least, largest):
    factor_of, own = 1.0, jax.random.fold_in(key, 6)
    for axis_at, blocks in pieces:
        steps = jnp.exp(jax.random.uniform(jax.random.fold_in(own, axis_at), (blocks,), jnp.float32, least / len(pieces), largest / len(pieces)))
        factor_of = factor_of * jnp.repeat(steps, shape[axis_at] // blocks).reshape([-1 if axis == axis_at else 1 for axis in range(len(shape))])
    return factor_of


def noise(stream_key, extent, spread, bound, cuts=(), kind=jnp.bfloat16):
    result = spread * jax.random.normal(stream_key, extent, jnp.float32)
    if cuts:
        result = result * block_scale(stream_key, extent, cuts, -0.22, 0.18)
    return jnp.clip(result, -bound, bound).astype(kind)


def setup_inputs(seed: int = 0) -> dict:
    arg_keys = jax.random.split(jax.random.key(seed), 6)
    return {
        "lookup_grads": noise(arg_keys[0], (LOOKUPS, EMB), 0.05, 0.29882812, ((0, 32),)),
        "slot_index": draw_slot_index(jax.random.fold_in(arg_keys[5], 71), 0),
        "unique_rows": draw_unique_rows(jax.random.fold_in(arg_keys[5], 71), 0),
        "tables": noise(arg_keys[3], (2, ROWS, EMB), 1.0, 6.0, ((1, 32),), jnp.float32),
        "accums": jnp.clip(jnp.exp(math.log(1.0) - 4.6051702 * jax.random.uniform(arg_keys[4], (2, ROWS), jnp.float32) ** block_scale(arg_keys[4], (2, ROWS), ((1, 32),), -0.2, 0.2)), 0.01, 1.0),
    }


learning_rate = 0.1
epsilon = 1e-08

def reference(lookup_grads, slot_index, unique_rows, tables, accums):
    per_group = LOOK_DEV * N_LOCAL
    grouped = lookup_grads.reshape(N_GROUP, per_group, EMB)
    slots_grouped = jnp.transpose(slot_index.reshape(2, N_GROUP, per_group), (1, 0, 2))

    def group_total(inputs):
        gradients, slots_here = inputs
        wide = gradients.astype(jnp.float32)
        first = jax.ops.segment_sum(wide, slots_here[0], num_segments=GROUP_SLOTS)
        second = jax.ops.segment_sum(wide, slots_here[1], num_segments=GROUP_SLOTS)
        return jnp.stack([first, second])
    group_sums = lax.map(group_total, (grouped, slots_grouped))
    group_sums = jnp.transpose(group_sums, (1, 0, 2, 3)).reshape(2, ALL_SLOTS, EMB)
    new_tables = []
    new_accums = []
    for table_index in range(2):
        row_numbers = unique_rows[table_index]
        targets = jnp.where(row_numbers < 0, ROWS, row_numbers).astype(jnp.int32)
        row_grads = jnp.zeros((ROWS, EMB), jnp.float32).at[targets].add(group_sums[table_index], mode='drop')
        accum_new = accums[table_index] + lax.optimization_barrier(jnp.mean(row_grads * row_grads, axis=1))
        table_new = tables[table_index] - learning_rate * row_grads / (jnp.sqrt(accum_new)[:, None] + epsilon)
        new_tables.append(table_new)
        new_accums.append(accum_new)
    return (jnp.stack(new_tables), jnp.stack(new_accums))
```

```python
import functools

import jax
import jax.numpy as jnp
from jax import lax
from jax.experimental import pallas as pl
from jax.experimental.pallas import tpu as pltpu
from jax.sharding import PartitionSpec as P

learning_rate = 0.1
epsilon = 1e-08
MESH = pl.DeviceIdType.MESH
BLOCKS = 4


def exchange_kernel(
    n_group, n_local, chunk, grads_hbm, index_ref, rows_ref, arrived_ref, rows_out_ref,
    grads, sums, recv, rows_recv, acc, grad_sems, send_sem, recv_sem, row_send_sem, row_recv_sem,
):
    group, local = lax.axis_index("group"), lax.axis_index("local")
    n_dev = n_group * n_local
    me = group * n_local + local
    look, width = grads.shape
    capacity = sums.shape[2]
    n_chunk = look // chunk
    locals_block = n_local // BLOCKS
    buckets = locals_block * n_group
    rows_block = buckets * capacity

    def load(k):
        at = pl.ds(k * chunk, chunk)
        return pltpu.make_async_copy(grads_hbm.at[at], grads.at[at], grad_sems.at[k])

    for k in range(n_chunk):
        load(k).start()

    barrier = pltpu.get_barrier_semaphore()

    def greet(o, c):
        to = lax.rem(me + o, n_dev)
        pl.semaphore_signal(
            barrier, inc=1, device_id={"group": to // n_local, "local": lax.rem(to, n_local)},
            device_id_type=MESH,
        )
        return c

    lax.fori_loop(1, n_dev, greet, 0)

    def send_bucket(bucket, l, h):
        return pltpu.make_async_remote_copy(
            src_ref=sums.at[bucket], dst_ref=recv.at[me],
            send_sem=send_sem, recv_sem=recv_sem,
            device_id={"group": h, "local": l}, device_id_type=MESH,
        )

    def send_rows(h):
        return pltpu.make_async_remote_copy(
            src_ref=rows_ref, dst_ref=rows_recv.at[group],
            send_sem=row_send_sem, recv_sem=row_recv_sem,
            device_id={"group": h, "local": local}, device_id_type=MESH,
        )

    block_me = local // locals_block
    for step in range(BLOCKS):
        block = lax.rem(block_me + (2, 1, 3, 0)[step], BLOCKS)
        targets = lax.broadcasted_iota(jnp.int32, (rows_block, chunk), 0) + block * rows_block
        acc[...] = jnp.zeros_like(acc)

        def body(k, c):
            if step == 0:
                load(k).wait()
            at = pl.ds(pl.multiple_of(k * chunk, chunk), chunk)
            onehot = jnp.concatenate(
                [jnp.where(index_ref[t : t + 1, at] == targets, 1.0, 0.0).astype(jnp.bfloat16) for t in range(2)],
                axis=0,
            )
            acc[...] += jnp.dot(onehot, grads[at, :], preferred_element_type=jnp.float32)
            return c

        lax.fori_loop(0, n_chunk, body, 0)
        first = block * buckets
        for t in range(2):
            sums[pl.ds(first, buckets), t] = acc[t * rows_block : (t + 1) * rows_block, :].reshape(
                buckets, capacity, width
            )
        if step == 0:
            pl.semaphore_wait(barrier, n_dev - 1)

            def row_step(o, c):
                send_rows(lax.rem(group + o, n_group)).start()
                return c

            lax.fori_loop(1, n_group, row_step, 0)

        if step < BLOCKS - 1:

            def out_step(i, c):
                l = block * locals_block + lax.rem(local + i // n_group, locals_block)
                h = lax.rem(group + i, n_group)
                send_bucket(l * n_group + h, l, h).start()
                return c

            lax.fori_loop(0, buckets, out_step, 0)
        else:

            def own_step(i, c):
                l = block * locals_block + lax.rem(local + i // n_group, locals_block)
                h = lax.rem(group + i, n_group)
                send_bucket(l * n_group + h, l, h).start()
                return c

            lax.fori_loop(1, buckets, own_step, 0)

    recv[me] = sums[local * n_group + group]
    rows_recv[group] = rows_ref[...]
    everyone = pltpu.make_async_remote_copy(
        src_ref=sums.at[pl.ds(0, n_dev - 1)], dst_ref=recv.at[pl.ds(0, n_dev - 1)],
        send_sem=send_sem, recv_sem=recv_sem,
        device_id={"group": group, "local": local}, device_id_type=MESH,
    )
    row_wait = pltpu.make_async_remote_copy(
        src_ref=rows_recv.at[pl.ds(0, n_group - 1)], dst_ref=rows_recv.at[pl.ds(0, n_group - 1)],
        send_sem=row_send_sem, recv_sem=row_recv_sem,
        device_id={"group": group, "local": local}, device_id_type=MESH,
    )
    row_wait.wait_recv()
    everyone.wait_recv()
    rows_out_ref[...] = rows_recv[...]
    for g in range(n_group):
        for t in range(2):
            total = recv[g * n_local, t]
            for l in range(1, n_local):
                total = total + recv[g * n_local + l, t]
            arrived_ref[t, g * capacity : (g + 1) * capacity, :] = total
    row_wait.wait_send()
    everyone.wait_send()


def update_kernel(
    n_group, rows_smem, rows_ref, arrived_ref, tables_ref, accums_ref, new_tables_ref, new_accums_ref, picked, fresh
):
    group, local = lax.axis_index("group"), lax.axis_index("local")
    n_local = lax.axis_size("local")
    rows_dev, width = tables_ref.shape[1:]
    slots = arrived_ref.shape[1]
    capacity = slots // n_group
    base = (group * n_local + local) * rows_dev
    new_tables_ref[...] = tables_ref[...]
    slot_at = lax.broadcasted_iota(jnp.int32, (capacity, slots), 0)
    lane_at = lax.broadcasted_iota(jnp.int32, (capacity, slots), 1)
    diagonal = lax.broadcasted_iota(jnp.int32, (slots, slots), 0) == lax.broadcasted_iota(jnp.int32, (slots, slots), 1)
    row_lane = lax.broadcasted_iota(jnp.int32, (slots, rows_dev), 1).astype(jnp.float32)
    for t in range(2):
        for s in range(slots):
            row = rows_smem[s // capacity, t, group * capacity + s % capacity]
            at = jnp.where(row < 0, 0, row - base)
            picked[s, :] = tables_ref[t, at, :]
        columns = []
        for g in range(n_group):
            mine = lane_at == slot_at + group * capacity
            ids = (rows_ref[g, t : t + 1, :]).astype(jnp.float32)
            columns.append(jnp.sum(jnp.where(mine, ids, 0.0), axis=1, keepdims=True))
        column = jnp.concatenate(columns, axis=0)
        as_row = jnp.sum(jnp.where(diagonal, column, 0.0), axis=0, keepdims=True)
        same = jnp.where(column == as_row, 1.0, 0.0)
        totals = jnp.dot(
            same, arrived_ref[t], preferred_element_type=jnp.float32, precision=lax.Precision.HIGHEST
        )
        squares = jnp.mean(totals * totals, axis=1, keepdims=True)
        local_row = jnp.where(column < 0.0, -1.0, column - base.astype(jnp.float32))
        hit = row_lane == local_row
        accums = accums_ref[t : t + 1, :]
        old = jnp.sum(jnp.where(hit, accums, 0.0), axis=1, keepdims=True)
        added = jnp.max(jnp.where(hit, squares, 0.0), axis=0, keepdims=True)
        new_accums_ref[t : t + 1, :] = accums + added
        fresh[...] = picked[...] - learning_rate * totals / (jnp.sqrt(old + squares) + epsilon)
        for s in range(slots):
            row = rows_smem[s // capacity, t, group * capacity + s % capacity]

            @pl.when(row >= 0)
            def _():
                new_tables_ref[t, row - base, :] = fresh[s, :]


def local_step(n_group, n_local, lookup_grads, slot_index, unique_rows, tables, accums):
    look, width = lookup_grads.shape
    slots = unique_rows.shape[1]
    capacity = slots // n_group
    n_dev = n_group * n_local
    chunk = min(1024, look)
    block_rows = 2 * (slots * n_local // BLOCKS)
    vmem = pl.BlockSpec(memory_space=pltpu.VMEM)
    dma = pltpu.SemaphoreType.DMA
    arrived, rows = pl.pallas_call(
        functools.partial(exchange_kernel, n_group, n_local, chunk),
        out_shape=(
            jax.ShapeDtypeStruct((2, slots, width), jnp.float32),
            jax.ShapeDtypeStruct((n_group, 2, slots), jnp.int32),
        ),
        in_specs=[pl.BlockSpec(memory_space=pl.ANY), vmem, vmem],
        out_specs=(vmem, vmem),
        scratch_shapes=[
            pltpu.VMEM((look, width), jnp.bfloat16),
            pltpu.VMEM((n_dev, 2, capacity, width), jnp.float32),
            pltpu.VMEM((n_dev, 2, capacity, width), jnp.float32),
            pltpu.VMEM((n_group, 2, slots), jnp.int32),
            pltpu.VMEM((block_rows, width), jnp.float32),
            dma((look // chunk,)), dma, dma, dma, dma,
        ],
        compiler_params=pltpu.CompilerParams(
            collective_id=0, has_side_effects=True, vmem_limit_bytes=40 * 2**20
        ),
        cost_estimate=pl.CostEstimate(flops=2 * 2 * look * width * slots * n_local, bytes_accessed=2 * look * width, transcendentals=0),
    )(lookup_grads, slot_index, unique_rows)
    return pl.pallas_call(
        functools.partial(update_kernel, n_group),
        out_shape=(
            jax.ShapeDtypeStruct(tables.shape, jnp.float32),
            jax.ShapeDtypeStruct(accums.shape, jnp.float32),
        ),
        in_specs=[pl.BlockSpec(memory_space=pltpu.SMEM), vmem, vmem, vmem, vmem],
        out_specs=(vmem, vmem),
        scratch_shapes=[pltpu.VMEM((slots, width), jnp.float32)] * 2,
        compiler_params=pltpu.CompilerParams(vmem_limit_bytes=24 * 2**20),
    )(rows, rows, arrived, tables, accums)


def solution(mesh):
    n_group, n_local = mesh.shape["group"], mesh.shape["local"]
    return jax.shard_map(
        functools.partial(local_step, n_group, n_local),
        mesh=mesh,
        in_specs=(
            P(("group", "local"), None),
            P(None, ("group", "local")),
            P(None, ("group", "local")),
            P(None, ("group", "local"), None),
            P(None, ("group", "local")),
        ),
        out_specs=(P(None, ("group", "local"), None), P(None, ("group", "local"))),
        check_vma=False,
    )
```

```python
import functools

import jax
import jax.numpy as jnp
from jax import lax
from jax.experimental import pallas as pl
from jax.experimental.pallas import tpu as pltpu
from jax.sharding import PartitionSpec as P

learning_rate = 0.1
epsilon = 1e-08
MESH = pl.DeviceIdType.MESH
BLOCKS = 4


def exchange_kernel(
    n_group, n_local, chunk, grads_hbm, index_hbm, rows_hbm, arrived_ref, rows_out_ref,
    grads, index, rows, sums, pair, recv, rows_recv, acc,
    grad_sems, index_sem, rows_sem, pair_sems, pair_send_sem, send_sem, recv_sem, row_send_sem, row_recv_sem,
):
    group, local = lax.axis_index("group"), lax.axis_index("local")
    n_dev = n_group * n_local
    me = group * n_local + local
    look, width = grads.shape
    capacity = sums.shape[2]
    n_chunk = look // chunk
    peers = n_local // BLOCKS
    buckets = peers * n_group
    rows_block = buckets * capacity
    block_me, peer_me = local // peers, lax.rem(local, peers)

    index_load = pltpu.make_async_copy(index_hbm, index, index_sem)
    rows_load = pltpu.make_async_copy(rows_hbm, rows, rows_sem)

    def load(k):
        at = pl.ds(k * chunk, chunk)
        return pltpu.make_async_copy(grads_hbm.at[at], grads.at[at], grad_sems.at[k])

    index_load.start()
    for k in range(n_chunk):
        load(k).start()
    rows_load.start()

    barrier = pltpu.get_barrier_semaphore()

    def greet(o, c):
        to = lax.rem(me + o, n_dev)
        pl.semaphore_signal(
            barrier, inc=1, device_id={"group": to // n_local, "local": lax.rem(to, n_local)},
            device_id_type=MESH,
        )
        return c

    lax.fori_loop(1, n_dev, greet, 0)

    def send_pair(block, o, h):
        to = block * peers + lax.rem(peer_me + o, peers)
        return pltpu.make_async_remote_copy(
            src_ref=sums.at[to * n_group + h],
            dst_ref=pair.at[(block * n_group + h) * (peers - 1) + (peers - 1 - o)],
            send_sem=pair_send_sem, recv_sem=pair_sems.at[block * n_group + h],
            device_id={"group": group, "local": block_me * peers + lax.rem(peer_me + o, peers)},
            device_id_type=MESH,
        )

    def send_bucket(l, h, place):
        return pltpu.make_async_remote_copy(
            src_ref=sums.at[l * n_group + h], dst_ref=recv.at[group * places + place],
            send_sem=send_sem, recv_sem=recv_sem,
            device_id={"group": h, "local": l}, device_id_type=MESH,
        )

    def send_rows(h):
        return pltpu.make_async_remote_copy(
            src_ref=rows, dst_ref=rows_recv.at[group],
            send_sem=row_send_sem, recv_sem=row_recv_sem,
            device_id={"group": h, "local": local}, device_id_type=MESH,
        )

    places = BLOCKS - 1 + peers
    order = (2, 1, 3, 0)

    def block_at(step):
        return lax.rem(block_me + order[step], BLOCKS)

    def sum_block(step):
        block = block_at(step)
        targets = lax.broadcasted_iota(jnp.int32, (rows_block, chunk), 0) + block * rows_block

        def body(k, c):
            if step == 0:
                load(k).wait()
            at = pl.ds(pl.multiple_of(k * chunk, chunk), chunk)
            onehot = jnp.concatenate(
                [jnp.where(index[t : t + 1, at] == targets, 1.0, 0.0).astype(jnp.bfloat16) for t in range(2)],
                axis=0,
            )
            acc[...] += jnp.dot(onehot, grads[at, :], preferred_element_type=jnp.float32)
            return c

        acc[...] = jnp.zeros_like(acc)
        if step == 0:
            index_load.wait()
        lax.fori_loop(0, n_chunk, body, 0)
        for t in range(2):
            sums[pl.ds(block * buckets, buckets), t] = acc[t * rows_block : (t + 1) * rows_block, :].reshape(
                buckets, capacity, width
            )

    def start_pairs(step):
        def one(i, c):
            send_pair(block_at(step), 1 + i // n_group, lax.rem(group + lax.rem(i, n_group), n_group)).start()
            return c

        lax.fori_loop(0, (peers - 1) * n_group, one, 0)

    def pass_on(step):
        block = block_at(step)
        mine = block * peers + peer_me

        def one(i, c):
            h = lax.rem(group + i, n_group)
            first = (block * n_group + h) * (peers - 1)
            pltpu.make_async_remote_copy(
                src_ref=pair.at[pl.ds(first, peers - 1)], dst_ref=pair.at[pl.ds(first, peers - 1)],
                send_sem=pair_send_sem, recv_sem=pair_sems.at[block * n_group + h],
                device_id={"group": group, "local": local}, device_id_type=MESH,
            ).wait_recv()
            total = sums[mine * n_group + h]
            for p in range(peers - 1):
                total = total + pair[first + p]
            sums[mine * n_group + h] = total
            send_bucket(mine, h, order[step] - 1).start()
            return c

        lax.fori_loop(0, n_group, one, 0)

    sum_block(0)
    pl.semaphore_wait(barrier, n_dev - 1)
    start_pairs(0)
    rows_load.wait()

    def row_step(o, c):
        send_rows(lax.rem(group + o, n_group)).start()
        return c

    lax.fori_loop(1, n_group, row_step, 0)
    for step in range(1, BLOCKS - 1):
        sum_block(step)
        start_pairs(step)
    pass_on(0)
    sum_block(BLOCKS - 1)

    def own_step(i, c):
        l = block_me * peers + lax.rem(peer_me + i // n_group, peers)
        send_bucket(l, lax.rem(group + i, n_group), BLOCKS - 1 + peer_me).start()
        return c

    lax.fori_loop(1, buckets, own_step, 0)
    for step in range(1, BLOCKS - 1):
        pass_on(step)

    recv[group * places + BLOCKS - 1 + peer_me] = sums[local * n_group + group]
    rows_recv[group] = rows[...]
    parts = n_group * places - 1
    everyone = pltpu.make_async_remote_copy(
        src_ref=recv.at[pl.ds(0, parts)], dst_ref=recv.at[pl.ds(0, parts)],
        send_sem=send_sem, recv_sem=recv_sem,
        device_id={"group": group, "local": local}, device_id_type=MESH,
    )
    row_wait = pltpu.make_async_remote_copy(
        src_ref=rows_recv.at[pl.ds(0, n_group - 1)], dst_ref=rows_recv.at[pl.ds(0, n_group - 1)],
        send_sem=row_send_sem, recv_sem=row_recv_sem,
        device_id={"group": group, "local": local}, device_id_type=MESH,
    )
    row_wait.wait_recv()
    rows_out_ref[...] = rows_recv[...]
    row_wait.wait_send()
    pair_wait_parts = (BLOCKS - 1) * n_group * (peers - 1)
    pltpu.make_async_remote_copy(
        src_ref=pair.at[pl.ds(0, pair_wait_parts)], dst_ref=pair.at[pl.ds(0, pair_wait_parts)],
        send_sem=pair_send_sem, recv_sem=recv_sem,
        device_id={"group": group, "local": local}, device_id_type=MESH,
    ).wait_send()
    everyone.wait_send()
    everyone.wait_recv()
    for g in range(n_group):
        for t in range(2):
            total = recv[g * places, t]
            for p in range(1, places):
                total = total + recv[g * places + p, t]
            arrived_ref[t, g * capacity : (g + 1) * capacity, :] = total


def update_kernel(
    n_group, rows_smem, rows_ref, arrived_ref, tables_ref, accums_ref, new_tables_hbm, new_accums_ref,
    picked, fresh, new, out_sems,
):
    group, local = lax.axis_index("group"), lax.axis_index("local")
    n_local = lax.axis_size("local")
    rows_dev, width = tables_ref.shape[1:]
    slots = arrived_ref.shape[1]
    capacity = slots // n_group
    base = (group * n_local + local) * rows_dev
    slot_at = lax.broadcasted_iota(jnp.int32, (capacity, slots), 0)
    lane_at = lax.broadcasted_iota(jnp.int32, (capacity, slots), 1)
    diagonal = lax.broadcasted_iota(jnp.int32, (slots, slots), 0) == lax.broadcasted_iota(jnp.int32, (slots, slots), 1)
    row_lane = lax.broadcasted_iota(jnp.int32, (slots, rows_dev), 1).astype(jnp.float32)

    def out(t):
        return pltpu.make_async_copy(new.at[t, pl.ds(0, rows_dev)], new_tables_hbm.at[t], out_sems.at[t])

    def row_of(t, s):
        return rows_smem[s // capacity, t, group * capacity + s % capacity]

    for t in range(2):
        new[t, 0:rows_dev] = tables_ref[t]
        for s in range(slots):
            row = row_of(t, s)
            picked[t, s, :] = tables_ref[t, jnp.where(row < 0, 0, row - base), :]
    for t in range(2):
        columns = []
        for g in range(n_group):
            mine = lane_at == slot_at + group * capacity
            ids = (rows_ref[g, t : t + 1, :]).astype(jnp.float32)
            columns.append(jnp.sum(jnp.where(mine, ids, 0.0), axis=1, keepdims=True))
        column = jnp.concatenate(columns, axis=0)
        as_row = jnp.sum(jnp.where(diagonal, column, 0.0), axis=0, keepdims=True)
        same = jnp.where(column == as_row, 1.0, 0.0)
        totals = jnp.dot(
            same, arrived_ref[t], preferred_element_type=jnp.float32, precision=lax.Precision.HIGHEST
        )
        squares = jnp.mean(totals * totals, axis=1, keepdims=True)
        local_row = jnp.where(column < 0.0, -1.0, column - base.astype(jnp.float32))
        hit = row_lane == local_row
        accums = accums_ref[t : t + 1, :]
        old = jnp.sum(jnp.where(hit, accums, 0.0), axis=1, keepdims=True)
        added = jnp.max(jnp.where(hit, squares, 0.0), axis=0, keepdims=True)
        new_accums_ref[t : t + 1, :] = accums + added
        fresh[t] = picked[t] - learning_rate * totals / (jnp.sqrt(old + squares) + epsilon)
        for s in range(slots):
            row = row_of(t, s)
            new[t, jnp.where(row < 0, rows_dev, row - base), :] = fresh[t, s, :]
        out(t).start()
    for t in range(2):
        out(t).wait()


def local_step(n_group, n_local, lookup_grads, slot_index, unique_rows, tables, accums):
    look, width = lookup_grads.shape
    slots = unique_rows.shape[1]
    capacity = slots // n_group
    n_dev = n_group * n_local
    rows_dev = tables.shape[1]
    chunk = min(4096, look)
    peers = n_local // BLOCKS
    block_rows = 2 * (slots * n_local // BLOCKS)
    vmem = pl.BlockSpec(memory_space=pltpu.VMEM)
    hbm = pl.BlockSpec(memory_space=pltpu.HBM)
    dma = pltpu.SemaphoreType.DMA
    arrived, rows = pl.pallas_call(
        functools.partial(exchange_kernel, n_group, n_local, chunk),
        out_shape=(
            jax.ShapeDtypeStruct((2, slots, width), jnp.float32),
            jax.ShapeDtypeStruct((n_group, 2, slots), jnp.int32),
        ),
        in_specs=[hbm, hbm, hbm],
        out_specs=(vmem, vmem),
        scratch_shapes=[
            pltpu.VMEM((look, width), jnp.bfloat16),
            pltpu.VMEM((2, look), jnp.int32),
            pltpu.VMEM((2, slots), jnp.int32),
            pltpu.VMEM((n_dev, 2, capacity, width), jnp.float32),
            pltpu.VMEM((BLOCKS * n_group * (peers - 1), 2, capacity, width), jnp.float32),
            pltpu.VMEM((n_group * (BLOCKS - 1 + peers), 2, capacity, width), jnp.float32),
            pltpu.VMEM((n_group, 2, slots), jnp.int32),
            pltpu.VMEM((block_rows, width), jnp.float32),
            dma((look // chunk,)), dma, dma, dma((BLOCKS * n_group,)), dma, dma, dma, dma, dma,
        ],
        compiler_params=pltpu.CompilerParams(
            collective_id=0, has_side_effects=True, vmem_limit_bytes=63 * 10**6
        ),
        cost_estimate=pl.CostEstimate(flops=2 * 2 * look * width * slots * n_local, bytes_accessed=2 * look * width, transcendentals=0),
    )(lookup_grads, slot_index, unique_rows)
    return pl.pallas_call(
        functools.partial(update_kernel, n_group),
        out_shape=(
            jax.ShapeDtypeStruct(tables.shape, jnp.float32),
            jax.ShapeDtypeStruct(accums.shape, jnp.float32),
        ),
        in_specs=[pl.BlockSpec(memory_space=pltpu.SMEM), vmem, vmem, vmem, vmem],
        out_specs=(hbm, vmem),
        scratch_shapes=[
            pltpu.VMEM((2, slots, width), jnp.float32),
            pltpu.VMEM((2, slots, width), jnp.float32),
            pltpu.VMEM((2, rows_dev + 8, width), jnp.float32),
            dma((2,)),
        ],
        compiler_params=pltpu.CompilerParams(vmem_limit_bytes=24 * 2**20),
    )(rows, rows, arrived, tables, accums)


def solution(mesh):
    n_group, n_local = mesh.shape["group"], mesh.shape["local"]
    return jax.shard_map(
        functools.partial(local_step, n_group, n_local),
        mesh=mesh,
        in_specs=(
            P(("group", "local"), None),
            P(None, ("group", "local")),
            P(None, ("group", "local")),
            P(None, ("group", "local"), None),
            P(None, ("group", "local")),
        ),
        out_specs=(P(None, ("group", "local"), None), P(None, ("group", "local"))),
        check_vma=False,
    )
```

```python
import functools

import jax
import jax.numpy as jnp
from jax import lax
from jax.experimental import pallas as pl
from jax.experimental.pallas import tpu as pltpu
from jax.sharding import PartitionSpec as P

learning_rate = 0.1
epsilon = 1e-08
MESH = pl.DeviceIdType.MESH
PIECES = 2
BLOCKS = 4


def exchange_kernel(
    n_group, n_local, chunk, grads_hbm, index_hbm, rows_hbm, packed_ref,
    grads, index, rows, sums, pair, recv, rows_recv, acc,
    grad_sems, index_sem, rows_sem, pair_sems, pair_send_sem, send_sem, recv_sem, row_send_sem, row_recv_sem,
):
    group, local = lax.axis_index("group"), lax.axis_index("local")
    n_dev = n_group * n_local
    me = group * n_local + local
    look, width = grads.shape
    capacity = sums.shape[2]
    n_chunk = look // chunk
    peers = n_local // BLOCKS
    buckets = peers * n_group
    rows_block = buckets * capacity
    block_me, peer_me = local // peers, lax.rem(local, peers)

    index_load = pltpu.make_async_copy(index_hbm, index, index_sem)
    rows_load = pltpu.make_async_copy(rows_hbm, rows, rows_sem)

    def load(k):
        at = pl.ds(k * chunk, chunk)
        return pltpu.make_async_copy(grads_hbm.at[at], grads.at[at], grad_sems.at[k])

    index_load.start()
    for k in range(n_chunk):
        load(k).start()
    rows_load.start()

    barrier = pltpu.get_barrier_semaphore()

    def greet(o, c):
        to = lax.rem(me + o, n_dev)
        pl.semaphore_signal(
            barrier, inc=1, device_id={"group": to // n_local, "local": lax.rem(to, n_local)},
            device_id_type=MESH,
        )
        return c

    lax.fori_loop(1, n_dev, greet, 0)

    def send_pair(block, o, h):
        to = block * peers + lax.rem(peer_me + o, peers)
        return pltpu.make_async_remote_copy(
            src_ref=sums.at[to * n_group + h],
            dst_ref=pair.at[(block * n_group + h) * (peers - 1) + (peers - 1 - o)],
            send_sem=pair_send_sem, recv_sem=pair_sems.at[block * n_group + h],
            device_id={"group": group, "local": block_me * peers + lax.rem(peer_me + o, peers)},
            device_id_type=MESH,
        )

    def send_bucket(l, h, place):
        return pltpu.make_async_remote_copy(
            src_ref=sums.at[l * n_group + h], dst_ref=recv.at[group * places + place],
            send_sem=send_sem, recv_sem=recv_sem,
            device_id={"group": h, "local": l}, device_id_type=MESH,
        )

    def send_rows(h):
        return pltpu.make_async_remote_copy(
            src_ref=rows, dst_ref=rows_recv.at[group],
            send_sem=row_send_sem, recv_sem=row_recv_sem,
            device_id={"group": h, "local": local}, device_id_type=MESH,
        )

    places = BLOCKS - 1 + peers
    order = (2, 1, 3, 0)

    def block_at(step):
        return lax.rem(block_me + order[step], BLOCKS)

    def sum_block(step):
        block = block_at(step)
        targets = lax.broadcasted_iota(jnp.int32, (rows_block, chunk), 0) + block * rows_block

        def body(k, c):
            if step == 0:
                load(k).wait()
            at = pl.ds(pl.multiple_of(k * chunk, chunk), chunk)
            onehot = jnp.concatenate(
                [jnp.where(index[t : t + 1, at] == targets, 1.0, 0.0).astype(jnp.bfloat16) for t in range(2)],
                axis=0,
            )
            acc[...] += jnp.dot(onehot, grads[at, :], preferred_element_type=jnp.float32)
            return c

        acc[...] = jnp.zeros_like(acc)
        if step == 0:
            index_load.wait()
        lax.fori_loop(0, n_chunk, body, 0)
        for t in range(2):
            sums[pl.ds(block * buckets, buckets), t] = acc[t * rows_block : (t + 1) * rows_block, :].reshape(
                buckets, capacity, width
            )

    def start_pairs(step):
        def one(i, c):
            send_pair(block_at(step), 1 + i // n_group, lax.rem(group + lax.rem(i, n_group), n_group)).start()
            return c

        lax.fori_loop(0, (peers - 1) * n_group, one, 0)

    def pass_on(step):
        block = block_at(step)
        mine = block * peers + peer_me

        def one(i, c):
            h = lax.rem(group + i, n_group)
            first = (block * n_group + h) * (peers - 1)
            pltpu.make_async_remote_copy(
                src_ref=pair.at[pl.ds(first, peers - 1)], dst_ref=pair.at[pl.ds(first, peers - 1)],
                send_sem=pair_send_sem, recv_sem=pair_sems.at[block * n_group + h],
                device_id={"group": group, "local": local}, device_id_type=MESH,
            ).wait_recv()
            total = sums[mine * n_group + h]
            for p in range(peers - 1):
                total = total + pair[first + p]
            sums[mine * n_group + h] = total
            send_bucket(mine, h, order[step] - 1).start()
            return c

        lax.fori_loop(0, n_group, one, 0)

    sum_block(0)
    pl.semaphore_wait(barrier, n_dev - 1)
    start_pairs(0)
    rows_load.wait()

    def row_step(o, c):
        send_rows(lax.rem(group + o, n_group)).start()
        return c

    lax.fori_loop(1, n_group, row_step, 0)
    for step in range(1, BLOCKS - 1):
        sum_block(step)
        start_pairs(step)
    pass_on(0)
    sum_block(BLOCKS - 1)

    def own_step(i, c):
        l = block_me * peers + lax.rem(peer_me + i // n_group, peers)
        send_bucket(l, lax.rem(group + i, n_group), BLOCKS - 1 + peer_me).start()
        return c

    lax.fori_loop(1, buckets, own_step, 0)
    for step in range(1, BLOCKS - 1):
        pass_on(step)

    recv[group * places + BLOCKS - 1 + peer_me] = sums[local * n_group + group]
    rows_recv[group] = rows[...]
    parts = n_group * places - 1
    everyone = pltpu.make_async_remote_copy(
        src_ref=recv.at[pl.ds(0, parts)], dst_ref=recv.at[pl.ds(0, parts)],
        send_sem=send_sem, recv_sem=recv_sem,
        device_id={"group": group, "local": local}, device_id_type=MESH,
    )
    row_wait = pltpu.make_async_remote_copy(
        src_ref=rows_recv.at[pl.ds(0, n_group - 1)], dst_ref=rows_recv.at[pl.ds(0, n_group - 1)],
        send_sem=row_send_sem, recv_sem=row_recv_sem,
        device_id={"group": group, "local": local}, device_id_type=MESH,
    )
    row_wait.wait_recv()
    slots = rows.shape[1]
    packed_ref[2 * slots :, :] = jnp.zeros_like(packed_ref[2 * slots :, :])
    for g in range(n_group):
        at = 2 * slots + 2 * g
        packed_ref[at : at + 2, 0:slots] = rows_recv[g].astype(jnp.float32)
    row_wait.wait_send()
    pair_wait_parts = (BLOCKS - 1) * n_group * (peers - 1)
    pltpu.make_async_remote_copy(
        src_ref=pair.at[pl.ds(0, pair_wait_parts)], dst_ref=pair.at[pl.ds(0, pair_wait_parts)],
        send_sem=pair_send_sem, recv_sem=recv_sem,
        device_id={"group": group, "local": local}, device_id_type=MESH,
    ).wait_send()
    everyone.wait_send()
    everyone.wait_recv()
    for g in range(n_group):
        for t in range(2):
            total = recv[g * places, t]
            for p in range(1, places):
                total = total + recv[g * places + p, t]
            at = t * slots + g * capacity
            packed_ref[at : at + capacity, :] = total


def update_kernel(n_group, slots, packed_ref, tables_ref, accums_ref, new_tables_hbm, new_accums_ref, new, out_sems):
    group, local = lax.axis_index("group"), lax.axis_index("local")
    n_local = lax.axis_size("local")
    rows_dev, width = tables_ref.shape[1:]
    capacity = slots // n_group
    base = ((group * n_local + local) * rows_dev).astype(jnp.float32)
    slot_at = lax.broadcasted_iota(jnp.int32, (capacity, slots), 0)
    lane_at = lax.broadcasted_iota(jnp.int32, (capacity, slots), 1)
    first_at = lax.broadcasted_iota(jnp.int32, (slots, slots), 0)
    second_at = lax.broadcasted_iota(jnp.int32, (slots, slots), 1)
    row_lane = lax.broadcasted_iota(jnp.int32, (slots, rows_dev), 1).astype(jnp.float32)
    piece = rows_dev // PIECES
    piece_row = lax.broadcasted_iota(jnp.int32, (piece, 3 * slots), 0).astype(jnp.float32)

    def out(t, i):
        at = pl.ds(i * piece, piece)
        return pltpu.make_async_copy(new.at[t, at], new_tables_hbm.at[t, at], out_sems.at[t, i])

    for t in range(2):
        columns = []
        for g in range(n_group):
            mine = lane_at == slot_at + group * capacity
            at = 2 * slots + 2 * g + t
            columns.append(jnp.sum(jnp.where(mine, packed_ref[at : at + 1, 0:slots], 0.0), axis=1, keepdims=True))
        column = jnp.concatenate(columns, axis=0)
        column = jnp.where(column < 0.0, -1.0, column - base)
        as_row = jnp.sum(jnp.where(first_at == second_at, column, 0.0), axis=0, keepdims=True)
        same = column == as_row
        totals = jnp.dot(
            jnp.where(same, 1.0, 0.0), packed_ref[t * slots : (t + 1) * slots, :],
            preferred_element_type=jnp.float32, precision=lax.Precision.HIGHEST,
        )
        squares = jnp.mean(totals * totals, axis=1, keepdims=True)
        hit = row_lane == column
        accums = accums_ref[t : t + 1, :]
        old = jnp.sum(jnp.where(hit, accums, 0.0), axis=1, keepdims=True)
        added = jnp.max(jnp.where(hit, squares, 0.0), axis=0, keepdims=True)
        new_accums_ref[t : t + 1, :] = accums + added
        change = learning_rate * totals / (jnp.sqrt(old + squares) + epsilon)
        earlier = jnp.max(jnp.where(same & (first_at < second_at), 1.0, 0.0), axis=0, keepdims=True)
        target = jnp.where(earlier > 0.0, -1.0, as_row)
        target = jnp.concatenate([target] * 3, axis=1)
        high = change.astype(jnp.bfloat16)
        rest = change - high.astype(jnp.float32)
        middle = rest.astype(jnp.bfloat16)
        low = (rest - middle.astype(jnp.float32)).astype(jnp.bfloat16)
        parts = jnp.concatenate([high, middle, low], axis=0)
        for i in range(PIECES):
            at = slice(i * piece, (i + 1) * piece)
            onehot = jnp.where(piece_row + float(i * piece) == target, 1.0, 0.0).astype(jnp.bfloat16)
            new[t, at] = tables_ref[t, at] - jnp.dot(onehot, parts, preferred_element_type=jnp.float32)
            out(t, i).start()
    for t in range(2):
        for i in range(PIECES):
            out(t, i).wait()


def local_step(n_group, n_local, lookup_grads, slot_index, unique_rows, tables, accums):
    look, width = lookup_grads.shape
    slots = unique_rows.shape[1]
    capacity = slots // n_group
    n_dev = n_group * n_local
    rows_dev = tables.shape[1]
    chunk = min(4096, look)
    peers = n_local // BLOCKS
    block_rows = 2 * (slots * n_local // BLOCKS)
    vmem = pl.BlockSpec(memory_space=pltpu.VMEM)
    hbm = pl.BlockSpec(memory_space=pltpu.HBM)
    dma = pltpu.SemaphoreType.DMA
    packed = pl.pallas_call(
        functools.partial(exchange_kernel, n_group, n_local, chunk),
        out_shape=jax.ShapeDtypeStruct((2 * slots + -(-2 * n_group // 8) * 8, width), jnp.float32),
        in_specs=[hbm, hbm, hbm],
        out_specs=vmem,
        scratch_shapes=[
            pltpu.VMEM((look, width), jnp.bfloat16),
            pltpu.VMEM((2, look), jnp.int32),
            pltpu.VMEM((2, slots), jnp.int32),
            pltpu.VMEM((n_dev, 2, capacity, width), jnp.float32),
            pltpu.VMEM((BLOCKS * n_group * (peers - 1), 2, capacity, width), jnp.float32),
            pltpu.VMEM((n_group * (BLOCKS - 1 + peers), 2, capacity, width), jnp.float32),
            pltpu.VMEM((n_group, 2, slots), jnp.int32),
            pltpu.VMEM((block_rows, width), jnp.float32),
            dma((look // chunk,)), dma, dma, dma((BLOCKS * n_group,)), dma, dma, dma, dma, dma,
        ],
        compiler_params=pltpu.CompilerParams(
            collective_id=0, has_side_effects=True, vmem_limit_bytes=63 * 10**6
        ),
        cost_estimate=pl.CostEstimate(flops=2 * 2 * look * width * slots * n_local, bytes_accessed=2 * look * width, transcendentals=0),
    )(lookup_grads, slot_index, unique_rows)
    return pl.pallas_call(
        functools.partial(update_kernel, n_group, slots),
        out_shape=(
            jax.ShapeDtypeStruct(tables.shape, jnp.float32),
            jax.ShapeDtypeStruct(accums.shape, jnp.float32),
        ),
        in_specs=[vmem, vmem, vmem],
        out_specs=(hbm, vmem),
        scratch_shapes=[
            pltpu.VMEM((2, rows_dev, width), jnp.float32),
            dma((2, PIECES)),
        ],
        compiler_params=pltpu.CompilerParams(vmem_limit_bytes=24 * 2**20),
    )(packed, tables, accums)


def solution(mesh):
    n_group, n_local = mesh.shape["group"], mesh.shape["local"]
    return jax.shard_map(
        functools.partial(local_step, n_group, n_local),
        mesh=mesh,
        in_specs=(
            P(("group", "local"), None),
            P(None, ("group", "local")),
            P(None, ("group", "local")),
            P(None, ("group", "local"), None),
            P(None, ("group", "local")),
        ),
        out_specs=(P(None, ("group", "local"), None), P(None, ("group", "local"))),
        check_vma=False,
    )
```

```python
import functools

import jax
import jax.numpy as jnp
from jax import lax
from jax.experimental import pallas as pl
from jax.experimental.pallas import tpu as pltpu
from jax.sharding import PartitionSpec as P

learning_rate = 0.1
epsilon = 1e-08
MESH = pl.DeviceIdType.MESH
PIECES = 2
BLOCKS = 4


def exchange_kernel(
    n_group, n_local, chunk, grads_hbm, index_hbm, rows_hbm, packed_ref,
    grads, index, rows, sums, pair, recv, rows_recv, acc,
    grad_sems, index_sem, rows_sem, pair_sems, pair_send_sem, send_sem, recv_sem, row_send_sem, row_recv_sem,
):
    group, local = lax.axis_index("group"), lax.axis_index("local")
    n_dev = n_group * n_local
    me = group * n_local + local
    look, width = grads.shape
    capacity = sums.shape[2]
    n_chunk = look // chunk
    peers = n_local // BLOCKS
    buckets = peers * n_group
    rows_block = buckets * capacity
    block_me, peer_me = local // peers, lax.rem(local, peers)

    index_load = pltpu.make_async_copy(index_hbm, index, index_sem)
    rows_load = pltpu.make_async_copy(rows_hbm, rows, rows_sem)

    def load(k):
        at = pl.ds(k * chunk, chunk)
        return pltpu.make_async_copy(grads_hbm.at[at], grads.at[at], grad_sems.at[k])

    index_load.start()
    for k in range(n_chunk):
        load(k).start()
    rows_load.start()

    barrier = pltpu.get_barrier_semaphore()

    def greet(o, c):
        to = lax.rem(me + o, n_dev)
        pl.semaphore_signal(
            barrier, inc=1, device_id={"group": to // n_local, "local": lax.rem(to, n_local)},
            device_id_type=MESH,
        )
        return c

    lax.fori_loop(1, n_dev, greet, 0)

    def send_pair(block, o, h):
        to = block * peers + lax.rem(peer_me + o, peers)
        return pltpu.make_async_remote_copy(
            src_ref=sums.at[to * n_group + h],
            dst_ref=pair.at[(block * n_group + h) * (peers - 1) + (peers - 1 - o)],
            send_sem=pair_send_sem, recv_sem=pair_sems.at[block * n_group + h],
            device_id={"group": group, "local": block_me * peers + lax.rem(peer_me + o, peers)},
            device_id_type=MESH,
        )

    def send_bucket(l, h, place):
        return pltpu.make_async_remote_copy(
            src_ref=sums.at[l * n_group + h], dst_ref=recv.at[group * places + place],
            send_sem=send_sem, recv_sem=recv_sem,
            device_id={"group": h, "local": l}, device_id_type=MESH,
        )

    def send_rows(h):
        return pltpu.make_async_remote_copy(
            src_ref=rows, dst_ref=rows_recv.at[group],
            send_sem=row_send_sem, recv_sem=row_recv_sem,
            device_id={"group": h, "local": local}, device_id_type=MESH,
        )

    places = BLOCKS - 1 + peers
    order = (2, 1, 3, 0)

    def block_at(step):
        return lax.rem(block_me + order[step], BLOCKS)

    def sum_block(step):
        block = block_at(step)
        targets = lax.broadcasted_iota(jnp.int32, (rows_block, chunk), 0) + block * rows_block

        def body(k, c):
            if step == 0:
                load(k).wait()
            at = pl.ds(pl.multiple_of(k * chunk, chunk), chunk)
            onehot = jnp.concatenate(
                [jnp.where(index[t : t + 1, at] == targets, 1.0, 0.0).astype(jnp.bfloat16) for t in range(2)],
                axis=0,
            )
            acc[...] += jnp.dot(onehot, grads[at, :], preferred_element_type=jnp.float32)
            return c

        acc[...] = jnp.zeros_like(acc)
        if step == 0:
            index_load.wait()
        lax.fori_loop(0, n_chunk, body, 0)
        for t in range(2):
            sums[pl.ds(block * buckets, buckets), t] = acc[t * rows_block : (t + 1) * rows_block, :].reshape(
                buckets, capacity, width
            )

    def start_pairs(step):
        def one(i, c):
            send_pair(block_at(step), 1 + i // n_group, lax.rem(group + lax.rem(i, n_group), n_group)).start()
            return c

        lax.fori_loop(0, (peers - 1) * n_group, one, 0)

    def pass_on(step, start, stop):
        block = block_at(step)
        mine = block * peers + peer_me

        def one(i, c):
            h = lax.rem(group + i, n_group)
            first = (block * n_group + h) * (peers - 1)
            pltpu.make_async_remote_copy(
                src_ref=pair.at[pl.ds(first, peers - 1)], dst_ref=pair.at[pl.ds(first, peers - 1)],
                send_sem=pair_send_sem, recv_sem=pair_sems.at[block * n_group + h],
                device_id={"group": group, "local": local}, device_id_type=MESH,
            ).wait_recv()
            total = sums[mine * n_group + h]
            for p in range(peers - 1):
                total = total + pair[first + p]
            sums[mine * n_group + h] = total
            send_bucket(mine, h, order[step] - 1).start()
            return c

        lax.fori_loop(start, stop, one, 0)

    sum_block(0)
    pl.semaphore_wait(barrier, n_dev - 1)
    start_pairs(0)
    rows_load.wait()

    def row_step(o, c):
        send_rows(lax.rem(group + o, n_group)).start()
        return c

    lax.fori_loop(1, n_group, row_step, 0)
    for step in range(1, BLOCKS - 1):
        sum_block(step)
        start_pairs(step)
        if step == 1:
            pass_on(0, 0, n_group // 2)
    pass_on(0, n_group // 2, n_group)
    sum_block(BLOCKS - 1)

    def own_step(i, c):
        l = block_me * peers + lax.rem(peer_me + i // n_group, peers)
        send_bucket(l, lax.rem(group + i, n_group), BLOCKS - 1 + peer_me).start()
        return c

    lax.fori_loop(1, buckets, own_step, 0)
    for step in range(1, BLOCKS - 1):
        pass_on(step, 0, n_group)

    recv[group * places + BLOCKS - 1 + peer_me] = sums[local * n_group + group]
    rows_recv[group] = rows[...]
    parts = n_group * places - 1
    everyone = pltpu.make_async_remote_copy(
        src_ref=recv.at[pl.ds(0, parts)], dst_ref=recv.at[pl.ds(0, parts)],
        send_sem=send_sem, recv_sem=recv_sem,
        device_id={"group": group, "local": local}, device_id_type=MESH,
    )
    row_wait = pltpu.make_async_remote_copy(
        src_ref=rows_recv.at[pl.ds(0, n_group - 1)], dst_ref=rows_recv.at[pl.ds(0, n_group - 1)],
        send_sem=row_send_sem, recv_sem=row_recv_sem,
        device_id={"group": group, "local": local}, device_id_type=MESH,
    )
    row_wait.wait_recv()
    slots = rows.shape[1]
    packed_ref[2 * slots :, :] = jnp.zeros_like(packed_ref[2 * slots :, :])
    for g in range(n_group):
        at = 2 * slots + 2 * g
        packed_ref[at : at + 2, 0:slots] = rows_recv[g].astype(jnp.float32)
    row_wait.wait_send()
    pair_wait_parts = (BLOCKS - 1) * n_group * (peers - 1)
    pltpu.make_async_remote_copy(
        src_ref=pair.at[pl.ds(0, pair_wait_parts)], dst_ref=pair.at[pl.ds(0, pair_wait_parts)],
        send_sem=pair_send_sem, recv_sem=recv_sem,
        device_id={"group": group, "local": local}, device_id_type=MESH,
    ).wait_send()
    everyone.wait_send()
    everyone.wait_recv()
    for g in range(n_group):
        for t in range(2):
            total = recv[g * places, t]
            for p in range(1, places):
                total = total + recv[g * places + p, t]
            at = t * slots + g * capacity
            packed_ref[at : at + capacity, :] = total


def update_kernel(n_group, slots, packed_ref, tables_ref, accums_ref, new_tables_hbm, new_accums_ref, new, out_sems):
    group, local = lax.axis_index("group"), lax.axis_index("local")
    n_local = lax.axis_size("local")
    rows_dev, width = tables_ref.shape[1:]
    capacity = slots // n_group
    base = ((group * n_local + local) * rows_dev).astype(jnp.float32)
    slot_at = lax.broadcasted_iota(jnp.int32, (capacity, slots), 0)
    lane_at = lax.broadcasted_iota(jnp.int32, (capacity, slots), 1)
    first_at = lax.broadcasted_iota(jnp.int32, (slots, slots), 0)
    second_at = lax.broadcasted_iota(jnp.int32, (slots, slots), 1)
    row_lane = lax.broadcasted_iota(jnp.int32, (slots, rows_dev), 1).astype(jnp.float32)
    piece = rows_dev // PIECES
    piece_row = lax.broadcasted_iota(jnp.int32, (piece, 3 * slots), 0).astype(jnp.float32)

    def out(t, i):
        at = pl.ds(i * piece, piece)
        return pltpu.make_async_copy(new.at[t, at], new_tables_hbm.at[t, at], out_sems.at[t, i])

    for t in range(2):
        columns = []
        for g in range(n_group):
            mine = lane_at == slot_at + group * capacity
            at = 2 * slots + 2 * g + t
            columns.append(jnp.sum(jnp.where(mine, packed_ref[at : at + 1, 0:slots], 0.0), axis=1, keepdims=True))
        column = jnp.concatenate(columns, axis=0)
        column = jnp.where(column < 0.0, -1.0, column - base)
        as_row = jnp.sum(jnp.where(first_at == second_at, column, 0.0), axis=0, keepdims=True)
        same = column == as_row
        totals = jnp.dot(
            jnp.where(same, 1.0, 0.0), packed_ref[t * slots : (t + 1) * slots, :],
            preferred_element_type=jnp.float32, precision=lax.Precision.HIGHEST,
        )
        squares = jnp.mean(totals * totals, axis=1, keepdims=True)
        hit = row_lane == column
        accums = accums_ref[t : t + 1, :]
        old = jnp.sum(jnp.where(hit, accums, 0.0), axis=1, keepdims=True)
        added = jnp.max(jnp.where(hit, squares, 0.0), axis=0, keepdims=True)
        new_accums_ref[t : t + 1, :] = accums + added
        change = learning_rate * totals / (jnp.sqrt(old + squares) + epsilon)
        earlier = jnp.max(jnp.where(same & (first_at < second_at), 1.0, 0.0), axis=0, keepdims=True)
        target = jnp.where(earlier > 0.0, -1.0, as_row)
        target = jnp.concatenate([target] * 3, axis=1)
        high = change.astype(jnp.bfloat16)
        rest = change - high.astype(jnp.float32)
        middle = rest.astype(jnp.bfloat16)
        low = (rest - middle.astype(jnp.float32)).astype(jnp.bfloat16)
        parts = jnp.concatenate([high, middle, low], axis=0)
        for i in range(PIECES):
            at = slice(i * piece, (i + 1) * piece)
            onehot = jnp.where(piece_row + float(i * piece) == target, 1.0, 0.0).astype(jnp.bfloat16)
            new[t, at] = tables_ref[t, at] - jnp.dot(onehot, parts, preferred_element_type=jnp.float32)
            out(t, i).start()
    for t in range(2):
        for i in range(PIECES):
            out(t, i).wait()


def local_step(n_group, n_local, lookup_grads, slot_index, unique_rows, tables, accums):
    look, width = lookup_grads.shape
    slots = unique_rows.shape[1]
    capacity = slots // n_group
    n_dev = n_group * n_local
    rows_dev = tables.shape[1]
    chunk = min(4096, look)
    peers = n_local // BLOCKS
    block_rows = 2 * (slots * n_local // BLOCKS)
    vmem = pl.BlockSpec(memory_space=pltpu.VMEM)
    hbm = pl.BlockSpec(memory_space=pltpu.HBM)
    dma = pltpu.SemaphoreType.DMA
    packed = pl.pallas_call(
        functools.partial(exchange_kernel, n_group, n_local, chunk),
        out_shape=jax.ShapeDtypeStruct((2 * slots + -(-2 * n_group // 8) * 8, width), jnp.float32),
        in_specs=[hbm, hbm, hbm],
        out_specs=vmem,
        scratch_shapes=[
            pltpu.VMEM((look, width), jnp.bfloat16),
            pltpu.VMEM((2, look), jnp.int32),
            pltpu.VMEM((2, slots), jnp.int32),
            pltpu.VMEM((n_dev, 2, capacity, width), jnp.float32),
            pltpu.VMEM((BLOCKS * n_group * (peers - 1), 2, capacity, width), jnp.float32),
            pltpu.VMEM((n_group * (BLOCKS - 1 + peers), 2, capacity, width), jnp.float32),
            pltpu.VMEM((n_group, 2, slots), jnp.int32),
            pltpu.VMEM((block_rows, width), jnp.float32),
            dma((look // chunk,)), dma, dma, dma((BLOCKS * n_group,)), dma, dma, dma, dma, dma,
        ],
        compiler_params=pltpu.CompilerParams(
            collective_id=0, has_side_effects=True, vmem_limit_bytes=63 * 10**6
        ),
        cost_estimate=pl.CostEstimate(flops=2 * 2 * look * width * slots * n_local, bytes_accessed=2 * look * width, transcendentals=0),
    )(lookup_grads, slot_index, unique_rows)
    return pl.pallas_call(
        functools.partial(update_kernel, n_group, slots),
        out_shape=(
            jax.ShapeDtypeStruct(tables.shape, jnp.float32),
            jax.ShapeDtypeStruct(accums.shape, jnp.float32),
        ),
        in_specs=[vmem, vmem, vmem],
        out_specs=(hbm, vmem),
        scratch_shapes=[
            pltpu.VMEM((2, rows_dev, width), jnp.float32),
            dma((2, PIECES)),
        ],
        compiler_params=pltpu.CompilerParams(vmem_limit_bytes=24 * 2**20),
    )(packed, tables, accums)


def solution(mesh):
    n_group, n_local = mesh.shape["group"], mesh.shape["local"]
    return jax.shard_map(
        functools.partial(local_step, n_group, n_local),
        mesh=mesh,
        in_specs=(
            P(("group", "local"), None),
            P(None, ("group", "local")),
            P(None, ("group", "local")),
            P(None, ("group", "local"), None),
            P(None, ("group", "local")),
        ),
        out_specs=(P(None, ("group", "local"), None), P(None, ("group", "local"))),
        check_vma=False,
    )
```
